32 devices in a mesh: dp: 16 (over z, y, core), tensor: 2 (over x).
Axes of the slice: x: 2, y: 2, z: 4, core: 2. Of those that a mesh axis runs over, the one named last changes fastest.
Arguments:
- training_token_input: bfloat16 [4096, 8192], P('dp', 'tensor'), may hold values from -6 to 6
- gate_output_gradient: bfloat16 [4096, 29568], P('dp', 'tensor'), may hold values from -6 to 6
- up_output_gradient: bfloat16 [4096, 29568], P('dp', 'tensor'), may hold values from -6 to 6
- gate_first_matrix: bfloat16 [8192, 64], P('tensor'), may hold values from -0.0625 to 0.0625
- gate_second_matrix: bfloat16 [64, 29568], P(None, 'tensor'), may hold values from -0.75 to 0.75
- up_first_matrix: bfloat16 [8192, 64], P('tensor'), may hold values from -0.0625 to 0.0625
- up_second_matrix: bfloat16 [64, 29568], P(None, 'tensor'), may hold values from -0.75 to 0.75
- gate_weight_base: bfloat16 [8192, 29568], P('tensor', 'dp'), may hold values from -0.0625 to 0.0625
- up_weight_base: bfloat16 [8192, 29568], P('tensor', 'dp'), may hold values from -0.0625 to 0.0625
- down_weight_base: bfloat16 [29568, 8192], P('dp', 'tensor'), may hold values from -0.03125 to 0.03125
- decode_step_input: bfloat16 [2, 512, 8192], P(None, None, 'tensor'), may hold values from -6 to 6
Outputs:
- decoded: bfloat16 [2, 512, 8192], P(None, None, 'tensor')
The draws below stay inside these ranges and needn't reach their ends.
All inputs are finite; a program needn't handle non-finite values.
Results may differ from the reference program's by a relative error of at most 0.04.
Values may be sent and summed in bfloat16 or wider, within the bound.
A program may use at most 192 MiB of HBM per device.

```python
import math
import jax
import jax.numpy as jnp
from jax import lax

MODEL_WIDTH = 8192
HIDDEN_UNITS = 29568
ADAPTER_RANK = 64
ROWS = 512
STEPS = 2
TOKENS = 4096
N_TENSOR = 2


def levels(own_key, shape, split, low, high):
    def one(dim, blocks):
        draws = jax.random.uniform(jax.random.fold_in(jax.random.fold_in(own_key, 6), dim), (blocks,), jnp.float32, low / len(split), high / len(split))
        return jnp.repeat(jnp.exp(draws), shape[dim] // blocks).reshape((-1,) + (1,) * (len(shape) - dim - 1))

    level = one(*split[0])
    for cut in split[1:]:
        level = level * one(*cut)
    return level


def centred(own_key, dims, scale, bound, cuts=(), kind=jnp.bfloat16):
    entries = jax.random.normal(own_key, dims, jnp.float32) * scale
    if len(cuts) > 0:
        entries = levels(own_key, dims, cuts, -0.22, 0.18) * entries
    return jnp.clip(entries, min=-bound, max=bound).astype(kind)


def setup_inputs(seed: int = 0) -> dict:
    splits = jax.random.split(jax.random.key(seed), 12)
    training_token_input = centred(splits[0], (TOKENS, MODEL_WIDTH), 1.0, 6.0, ((0, 16), (1, 2)))
    gate_output_gradient = centred(splits[1], (TOKENS, HIDDEN_UNITS), 1.0, 6.0, ((0, 16), (1, 2)))
    up_output_gradient = centred(splits[2], (TOKENS, HIDDEN_UNITS), 1.0, 6.0, ((0, 16), (1, 2)))
    gate_first_matrix = centred(splits[3], (MODEL_WIDTH, ADAPTER_RANK), MODEL_WIDTH ** -0.5, 0.0625, ((0, 2),))
    gate_second_matrix = centred(splits[4], (ADAPTER_RANK, HIDDEN_UNITS), ADAPTER_RANK ** -0.5, 0.75, ((1, 2),))
    up_first_matrix = centred(splits[5], (MODEL_WIDTH, ADAPTER_RANK), MODEL_WIDTH ** -0.5, 0.0625, ((0, 2),))
    up_second_matrix = centred(splits[6], (ADAPTER_RANK, HIDDEN_UNITS), ADAPTER_RANK ** -0.5, 0.75, ((1, 2),))
    gate_weight_base = centred(splits[7], (MODEL_WIDTH, HIDDEN_UNITS), MODEL_WIDTH ** -0.5, 0.0625, ((0, 2), (1, 16)))
    up_weight_base = centred(splits[8], (MODEL_WIDTH, HIDDEN_UNITS), MODEL_WIDTH ** -0.5, 0.0625, ((0, 2), (1, 16)))
    down_weight_base = centred(splits[9], (HIDDEN_UNITS, MODEL_WIDTH), HIDDEN_UNITS ** -0.5, 0.03125, ((0, 16), (1, 2)))
    decode_step_input = centred(splits[10], (STEPS, ROWS, MODEL_WIDTH), 1.0, 6.0, ((2, 2),))
    return {"training_token_input": training_token_input, "gate_output_gradient": gate_output_gradient, "up_output_gradient": up_output_gradient, "gate_first_matrix": gate_first_matrix, "gate_second_matrix": gate_second_matrix, "up_first_matrix": up_first_matrix, "up_second_matrix": up_second_matrix, "gate_weight_base": gate_weight_base, "up_weight_base": up_weight_base, "down_weight_base": down_weight_base, "decode_step_input": decode_step_input}


def partial_rounded(inputs, weight):
    blocks = jnp.moveaxis(inputs.reshape(inputs.shape[0], N_TENSOR, -1), 1, 0)
    pieces = weight.reshape(N_TENSOR, -1, weight.shape[1])

    def one_block(pair):
        left, right = pair
        total = jnp.dot(left, right, preferred_element_type=jnp.float32)
        return lax.optimization_barrier(total.astype(jnp.bfloat16)).astype(jnp.float32)
    terms = lax.map(one_block, (blocks, pieces))
    return lax.optimization_barrier(jnp.sum(terms, axis=0))

def reference(training_token_input, gate_output_gradient, up_output_gradient, gate_first_matrix, gate_second_matrix, up_first_matrix, up_second_matrix, gate_weight_base, up_weight_base, down_weight_base, decode_step_input):
    second_learning_rate = 0.5 / math.sqrt(ADAPTER_RANK * TOKENS)
    first_learning_rate = 0.5 / math.sqrt(MODEL_WIDTH * HIDDEN_UNITS * TOKENS / ADAPTER_RANK)

    def apply_adapter(cotangent, factor_b, factor_a, base):
        inner_b = jnp.dot(training_token_input, factor_b, preferred_element_type=jnp.float32).astype(jnp.bfloat16)
        inner_a = jnp.dot(cotangent, factor_a.T, preferred_element_type=jnp.float32).astype(jnp.bfloat16)
        grad_a = jnp.dot(inner_b.T, cotangent, preferred_element_type=jnp.float32)
        grad_b = jnp.dot(training_token_input.T, inner_a, preferred_element_type=jnp.float32)
        fresh_b = (factor_b.astype(jnp.float32) - first_learning_rate * grad_b).astype(jnp.bfloat16)
        fresh_a = (factor_a.astype(jnp.float32) - second_learning_rate * grad_a).astype(jnp.bfloat16)
        update = jnp.dot(fresh_b, fresh_a, preferred_element_type=jnp.float32)
        return (base.astype(jnp.float32) + update).astype(jnp.bfloat16)
    combined_gate_weight = apply_adapter(gate_output_gradient, gate_first_matrix, gate_second_matrix, gate_weight_base)
    combined_up_weight = apply_adapter(up_output_gradient, up_first_matrix, up_second_matrix, up_weight_base)
    results = []
    for position in range(STEPS):
        rows_in = decode_step_input[position]
        gate = partial_rounded(rows_in, combined_gate_weight)
        upper = partial_rounded(rows_in, combined_up_weight)
        hidden = (jax.nn.silu(gate) * upper).astype(jnp.bfloat16)
        results.append(jnp.dot(hidden, down_weight_base, preferred_element_type=jnp.float32).astype(jnp.bfloat16))
    return jnp.stack(results)
```

```python
import math

import jax
import jax.numpy as jnp
from jax import lax
from jax.sharding import PartitionSpec as P

MODEL_WIDTH = 8192
HIDDEN_UNITS = 29568
ADAPTER_RANK = 64


def swap(value):
    return lax.ppermute(value, "tensor", ((0, 1), (1, 0)))


def pair_sum(value):
    if lax.axis_size("tensor") == 2:
        sent = value.astype(jnp.bfloat16)
        return sent.astype(jnp.float32) + swap(sent).astype(jnp.float32)
    return lax.psum(value.astype(jnp.bfloat16), "tensor").astype(jnp.float32)


def row_share(value, index):
    rows = value.shape[1] // lax.axis_size("tensor")
    return lax.dynamic_slice_in_dim(value, index * rows, rows, 1)


def on_device(
    training_token_input,
    gate_output_gradient,
    up_output_gradient,
    gate_first_matrix,
    gate_second_matrix,
    up_first_matrix,
    up_second_matrix,
    gate_weight_base,
    up_weight_base,
    down_weight_base,
    decode_step_input,
):
    f32, bf16 = jnp.float32, jnp.bfloat16
    n_dp, n_tensor = lax.axis_size("dp"), lax.axis_size("tensor")
    me = lax.axis_index("tensor")
    replica = lax.axis_index("dp")
    rank = gate_first_matrix.shape[1]
    tokens_total = training_token_input.shape[0] * n_dp
    second_learning_rate = 0.5 / math.sqrt(ADAPTER_RANK * tokens_total)
    first_learning_rate = 0.5 / math.sqrt(MODEL_WIDTH * HIDDEN_UNITS * tokens_total / ADAPTER_RANK)

    def dot(left, right, over):
        return lax.dot_general(left, right, (over, ((), ())), preferred_element_type=f32)

    firsts = jnp.concatenate([gate_first_matrix, up_first_matrix], axis=1)
    inner = jnp.concatenate(
        [
            jnp.dot(training_token_input, firsts, preferred_element_type=f32),
            dot(gate_output_gradient, gate_second_matrix, ((1,), (1,))),
            dot(up_output_gradient, up_second_matrix, ((1,), (1,))),
        ],
        axis=1,
    )
    inner = pair_sum(inner).astype(bf16)
    inner_b, inner_a = inner[:, : 2 * rank], inner[:, 2 * rank :]

    columns = gate_weight_base.shape[1]
    group = n_dp // n_tensor
    unit = 16 * n_tensor
    padded = -(-columns // unit) * unit
    piece = padded // n_tensor
    second_gradient = jnp.concatenate(
        [
            dot(gate_output_gradient, inner_b[:, :rank], ((0,), (0,))).astype(bf16),
            dot(up_output_gradient, inner_b[:, rank:], ((0,), (0,))).astype(bf16),
        ],
        axis=1,
    )
    second_gradient = jnp.pad(
        second_gradient.reshape(group, columns, 2 * rank),
        ((0, 0), (0, padded - columns), (0, 0)),
    ).reshape(group * padded, 2 * rank)
    first_gradient = dot(training_token_input, inner_a, ((0,), (0,))).astype(bf16)

    rows_in, second_gradient, first_gradient = lax.optimization_barrier(
        (decode_step_input, second_gradient, first_gradient)
    )
    second_gradient = lax.psum_scatter(second_gradient, "dp", scatter_dimension=0, tiled=True)
    first_gradient = lax.psum(first_gradient, "dp")

    def base(rows, weight):
        return dot(rows, weight, ((2,), (0,))).astype(bf16)

    weights = (gate_weight_base, up_weight_base)
    if n_tensor == 2:
        theirs = row_share(rows_in, 1 - me)
        ours = row_share(rows_in, me)
        arrived = [swap(base(theirs, weight)) for weight in weights]
        base_sums = [
            base(ours, weight).astype(f32) + other.astype(f32)
            for weight, other in zip(weights, arrived)
        ]
    else:
        base_sums = [
            lax.psum_scatter(
                base(rows_in, weight), "tensor", scatter_dimension=1, tiled=True
            ).astype(f32)
            for weight in weights
        ]

    start = replica // n_tensor * columns + replica % n_tensor * piece

    def old_piece(matrix):
        wide = jnp.pad(matrix, ((0, 0), (0, padded)))
        return lax.dynamic_slice_in_dim(wide, start, piece, 1).T

    old = jnp.concatenate([old_piece(gate_second_matrix), old_piece(up_second_matrix)], axis=1)
    stepped = (
        old.astype(f32) - second_learning_rate * second_gradient.astype(f32)
    ).astype(bf16)
    routes = [
        (
            (block * n_tensor + part) * n_tensor + side,
            (side * group + block) * n_tensor + part,
        )
        for block in range(group)
        for part in range(n_tensor)
        for side in range(n_tensor)
    ]
    stepped = lax.ppermute(stepped, ("dp", "tensor"), routes)
    if n_tensor == 2:
        other = swap(stepped)
        first_half = me == 0
        seconds = jnp.concatenate(
            [jnp.where(first_half, stepped, other), jnp.where(first_half, other, stepped)], axis=0
        )
    else:
        seconds = lax.all_gather(stepped, "tensor", axis=0, tiled=True)
    seconds = seconds[:columns]

    new_firsts = (
        firsts.astype(f32) - first_learning_rate * first_gradient.astype(f32)
    ).astype(bf16)
    low = dot(rows_in, new_firsts, ((2,), (0,)))
    if n_tensor == 2:
        low = row_share(low, me) + swap(row_share(low, 1 - me).astype(bf16)).astype(f32)
    else:
        low = lax.psum_scatter(
            low.astype(bf16), "tensor", scatter_dimension=1, tiled=True
        ).astype(f32)
    low = low.astype(bf16)

    gate = base_sums[0] + dot(low[..., :rank], seconds[:, :rank], ((2,), (1,)))
    upper = base_sums[1] + dot(low[..., rank:], seconds[:, rank:], ((2,), (1,)))
    hidden = (jax.nn.silu(gate) * upper).astype(bf16)

    def project(part):
        steps, rows, _ = part.shape
        out = dot(part, down_weight_base, ((2,), (0,))).astype(bf16)
        out = out.reshape(steps * rows, -1)
        out = lax.psum_scatter(out, "dp", scatter_dimension=0, tiled=True)
        out = lax.all_gather(out, "dp", axis=0, tiled=True)
        return out.reshape(steps, rows, -1)

    if n_tensor == 2:
        own = project(hidden)
        other = project(swap(hidden))
        share = hidden.shape[1]
        result = jnp.zeros(decode_step_input.shape[:2] + (own.shape[2],), bf16)
        result = lax.dynamic_update_slice_in_dim(result, own, me * share, 1)
        return lax.dynamic_update_slice_in_dim(result, other, (1 - me) * share, 1)
    return project(lax.all_gather(hidden, "tensor", axis=1, tiled=True))


def solution(mesh):
    placed = (
        P("dp", "tensor"),
        P("dp", "tensor"),
        P("dp", "tensor"),
        P("tensor", None),
        P(None, "tensor"),
        P("tensor", None),
        P(None, "tensor"),
        P("tensor", "dp"),
        P("tensor", "dp"),
        P("dp", "tensor"),
        P(None, None, "tensor"),
    )
    return jax.shard_map(
        on_device, mesh=mesh, in_specs=placed, out_specs=P(None, None, "tensor"), check_vma=False
    )
```
